32 devices in a mesh: day: 8 (over y, x, core), pair: 4 (over z).
Axes of the slice: x: 2, y: 2, z: 4, core: 2. Of those that a mesh axis runs over, the one named last changes fastest.
Arguments:
- correlations: bfloat16 [32, 2048, 2001], P('day', 'pair'), may hold values from -8 to 8
- mask: int32 [32, 2048], P('day', 'pair'), may hold values from 0 to 1, as said below
- counts: int32 [2048], P(('pair', 'day')), may hold values from 1 to 32, as said below
Outputs:
- phase_weighted: float32 [2048, 2001], P(('pair', 'day'))
- linear: float32 [2048, 2001], P(('pair', 'day'))
The draws below stay inside these ranges and needn't reach their ends.
Inputs may be any that keep to these rules, and one draw needn't show every extreme that they name: `mask`: every pair has a usable correlation on at least one day. counts[p] equals the number of days d with mask[d, p] = 1.
All inputs are finite; a program needn't handle non-finite values.
Results may differ from the reference program's by a relative error of at most 0.00044.
Values may be sent and summed in bfloat16 or wider, within the bound.
A program may use at most 128 MiB of HBM per device.

```python
import jax
import jax.numpy as jnp
from jax import lax

LAGS = 2001
DAYS = 32
PAIRS = 2048


def mask_pair(key):
    base = jax.random.fold_in(key, 7)
    keys = jax.random.split(base, 5)
    day_rate = jax.random.randint(keys[0], (DAYS,), 30, 101)
    pair_rate = jax.random.randint(keys[1], (PAIRS,), 40, 101)
    draws = jax.random.randint(keys[2], (DAYS, PAIRS), 0, 10000)
    usable = (draws < day_rate[:, None] * pair_rate[None, :]).astype(jnp.int32)
    forced = jax.random.randint(keys[3], (PAIRS,), 0, DAYS)
    chosen = (jnp.arange(DAYS)[:, None] == forced[None, :]).astype(jnp.int32)
    usable = jnp.maximum(usable, chosen)
    full_pair = jax.random.randint(keys[4], (), 0, PAIRS)
    always = (jnp.arange(PAIRS) == full_pair).astype(jnp.int32)
    usable = jnp.maximum(usable, always[None, :])
    return (usable, jnp.sum(usable, axis=0).astype(jnp.int32))


def draw_mask(key, part):
    return mask_pair(key)[0]


def draw_counts(key, part):
    return mask_pair(key)[1]


def draw_correlations(key, part):
    keys = jax.random.split(jax.random.fold_in(key, 3), 5)
    block_index = jnp.arange(PAIRS) // 64
    block_total = (PAIRS + 63) // 64
    pair_scale = jnp.exp(jax.random.uniform(keys[0], (PAIRS,), jnp.float32, -0.8, 0.8))
    block_scale = jnp.exp(jax.random.uniform(keys[1], (block_total,), jnp.float32, -0.8, 0.8))[block_index]
    day_scale = jnp.exp(jax.random.uniform(keys[2], (DAYS,), jnp.float32, -0.7, 0.7))
    signal = 0.7 * jax.random.normal(keys[3], (PAIRS, LAGS), jnp.float32)
    noise = jax.random.normal(keys[4], (DAYS, PAIRS, LAGS), jnp.float32)
    values = day_scale[:, None, None] * (pair_scale * block_scale)[None, :, None] * (signal[None] + noise)
    return jnp.clip(values, -8.0, 8.0).astype(jnp.bfloat16)


def setup_inputs(seed: int = 0) -> dict:
    seeds = jax.random.split(jax.random.key(seed), 4)
    correlations = draw_correlations(jax.random.fold_in(seeds[3], 71), 0)
    mask = draw_mask(jax.random.fold_in(seeds[3], 71), 0)
    counts = draw_counts(jax.random.fold_in(seeds[3], 71), 0)
    return dict(correlations=correlations, mask=mask, counts=counts)


def hilbert_kernel():
    offset = jnp.arange(LAGS, dtype=jnp.int32)
    offset = jnp.where(offset > LAGS // 2, offset - LAGS, offset)
    phase_angle = jnp.pi * offset.astype(jnp.float32) / LAGS
    parity = 1.0 - 2.0 * (offset % 2).astype(jnp.float32)
    sine_safe = jnp.where(offset == 0, 1.0, jnp.sin(phase_angle))
    kernel = jnp.where(offset == 0, 0.0, (jnp.cos(phase_angle) - parity) / (LAGS * sine_safe))
    rounded = lax.optimization_barrier(kernel.astype(jnp.bfloat16))
    return rounded.astype(jnp.float32)

def hilbert_part(day_rows, kernel_spectrum):
    spectrum = jnp.fft.fft(day_rows, axis=-1)
    return jnp.real(jnp.fft.ifft(spectrum * kernel_spectrum, axis=-1))

def reference(correlations, mask, counts):
    masked = correlations * mask[:, :, None].astype(jnp.bfloat16)
    energy = lax.map(lambda day_rows: jnp.sum(jnp.square(day_rows.astype(jnp.float32))), masked)
    used_pairs = lax.optimization_barrier(jnp.sum(mask, axis=1)).astype(jnp.float32)
    weight = 1.0 / jnp.sqrt(energy / (LAGS * jnp.maximum(used_pairs, 1.0)) + 0.1)
    kernel_spectrum = jnp.fft.fft(hilbert_kernel())

    def add_day(totals, inputs):
        day_rows, day_weight = inputs
        values = day_rows.astype(jnp.float32)
        real_part = day_weight * values
        imag_part = day_weight * hilbert_part(values, kernel_spectrum)
        amplitude = jnp.sqrt(real_part * real_part + imag_part * imag_part + 0.25)
        return ((totals[0] + real_part, totals[1] + real_part / amplitude, totals[2] + imag_part / amplitude), None)
    zeros = jnp.zeros((PAIRS, LAGS), jnp.float32)
    totals, unused = lax.scan(add_day, (zeros, zeros, zeros), (masked, weight))
    divisor = jnp.maximum(counts.astype(jnp.float32), 1.0)[:, None]
    linear = totals[0] / divisor
    coherence = (totals[1] * totals[1] + totals[2] * totals[2]) / (divisor * divisor)
    return (linear * coherence, linear)
```

```python
import functools

import jax
import jax.numpy as jnp
import numpy as np
from jax import lax
from jax.experimental import pallas as pl
from jax.experimental.pallas import tpu as pltpu
from jax.sharding import PartitionSpec as P

TILE = 256
FULL = 32767.0
UNIT = 2.0**20


def padded(lag_count):
    return -(-lag_count // TILE) * TILE


def kernel_strip(lag_count):
    f32 = np.float32
    offset = np.arange(lag_count, dtype=np.int32)
    offset = np.where(offset > lag_count // 2, offset - lag_count, offset)
    angle = f32(np.pi) * offset.astype(f32) / f32(lag_count)
    parity = f32(1) - f32(2) * (offset % 2).astype(f32)
    sine = np.where(offset == 0, f32(1), np.sin(angle)).astype(f32)
    kernel = np.where(offset == 0, f32(0), (np.cos(angle) - parity) / (f32(lag_count) * sine))
    width = padded(lag_count)
    index = np.arange(2 * width - TILE)[None, :] - np.arange(TILE)[:, None] - (width - TILE)
    return kernel.astype(f32)[index % lag_count].astype(jnp.bfloat16)


def codes(values):
    top = jnp.max(jnp.abs(values), axis=1, keepdims=True)
    units = (top * UNIT).astype(jnp.int32) + 1
    step = FULL * UNIT / units.astype(jnp.float32)
    return jnp.round(values * step).astype(jnp.int32), units


def join(high, low):
    return high * 65536 + (low & 65535)


def split(word):
    low = ((word & 65535) ^ 32768) - 32768
    return word >> 16, low


def stack_kernel(lag_count, mine_ref, other_ref, scale_ref, strip_ref, out_ref, table, rows_ref, sums):
    width = table.shape[1]
    days, rows = mine_ref.shape[0], mine_ref.shape[1]
    total = 2 * days * rows
    last = width - TILE

    @pl.when(pl.program_id(0) == 0)
    def _():
        for i in range(width // TILE):
            start = width - TILE - i * TILE
            table[pl.ds(i * TILE, TILE), :] = strip_ref[:, start : start + width]
        col = lax.broadcasted_iota(jnp.int32, (width, TILE), 1) + last
        table[:, last:] = jnp.where(col < lag_count, table[:, last:], jnp.zeros_like(table[:, last:]))

    lane = lax.broadcasted_iota(jnp.int32, (days * rows, TILE), 1) + last
    for part, ref in enumerate((mine_ref, other_ref)):
        there = pl.ds(part * days * rows, days * rows)
        rows_ref[there, :last] = ref[:, :, :last].reshape(days * rows, last)
        tail = ref[:, :, last:].reshape(days * rows, TILE)
        rows_ref[there, last:] = jnp.where(lane < lag_count, tail, jnp.zeros_like(tail))

    scale = scale_ref[...].reshape(total, 1)
    for j in range(width // TILE):
        cols = slice(j * TILE, (j + 1) * TILE)
        hilbert = jnp.dot(rows_ref[...], table[:, cols], preferred_element_type=jnp.float32)
        real = scale * rows_ref[:, cols].astype(jnp.float32)
        imag = scale * hilbert
        inverse = lax.rsqrt(real * real + imag * imag + 0.25)
        for k, term in enumerate((real, real * inverse, imag * inverse)):
            sums[k, :, cols] = jnp.sum(term.reshape(2 * days, rows, TILE), axis=0)
    half = width // 2
    linear, linear_units = codes(sums[0])
    first, first_units = codes(sums[1])
    second, second_units = codes(sums[2])
    out_ref[0, :, :width] = join(first, second)
    out_ref[0, :, width : width + half] = join(linear[:, :half], linear[:, half:])
    pick = lax.broadcasted_iota(jnp.int32, (rows, 128), 1)
    out_ref[0, :, width + half :] = jnp.where(
        pick == 0, linear_units, jnp.where(pick == 1, first_units, second_units)
    )


def finish_kernel(lag_count, words_ref, counts_ref, weighted_ref, linear_ref):
    parts, rows, size = words_ref.shape
    width = (size - 128) * 2 // 3
    half = width // 2
    linear = real = imag = 0.0
    for k in range(parts):
        units = words_ref[k, :, width + half :].astype(jnp.float32) * (1.0 / (FULL * UNIT))
        first, second = split(words_ref[k, :, :width])
        left, right = split(words_ref[k, :, width : width + half])
        both = jnp.concatenate([left, right], axis=1)
        linear += both.astype(jnp.float32) * units[:, 0:1]
        real += first.astype(jnp.float32) * units[:, 1:2]
        imag += second.astype(jnp.float32) * units[:, 2:3]
    inverse = 1.0 / jnp.maximum(counts_ref[...].astype(jnp.float32), 1.0)
    linear = linear * inverse
    weighted = linear * ((real * real + imag * imag) * (inverse * inverse))
    linear_ref[...] = linear[:, :lag_count]
    weighted_ref[...] = weighted[:, :lag_count]


def shards(correlations, mask, counts):
    days, pairs, lag_count = correlations.shape
    groups = lax.axis_size("day")
    me = lax.axis_index("day")
    core = me % 2
    owned = pairs // groups
    width = padded(lag_count)

    squares = jnp.sum(jnp.square(correlations.astype(jnp.float32)), axis=2)
    mask_f = mask.astype(jnp.float32)
    local = jnp.stack([jnp.sum(squares * mask_f, axis=1), jnp.sum(mask_f, axis=1)])
    slots = lax.dynamic_update_slice(jnp.zeros((2, groups * days), jnp.float32), local, (0, me * days))
    energy, used = lax.psum(slots, ("day", "pair"))
    weight = lax.rsqrt(energy / (lag_count * jnp.maximum(used, 1.0)) + 0.1)

    couple = [(i, i ^ 1) for i in range(groups)]
    blocks = correlations.reshape(days, groups // 2, 2, owned, lag_count)
    mask_blocks = mask_f.reshape(days, groups // 2, 2, owned)
    mine, other = (jnp.where(core == 0, blocks[:, :, s], blocks[:, :, 1 - s]) for s in (0, 1))
    mask_mine, mask_other = (jnp.where(core == 0, mask_blocks[:, :, s], mask_blocks[:, :, 1 - s]) for s in (0, 1))
    other = lax.ppermute(other, "day", couple)
    mask_other = lax.ppermute(mask_other, "day", couple)

    weight_mine = lax.dynamic_slice(weight, (me * days,), (days,))
    weight_other = lax.dynamic_slice(weight, ((me ^ 1) * days,), (days,))
    scale = jnp.concatenate(
        [mask_mine * weight_mine[:, None, None], mask_other * weight_other[:, None, None]], axis=0
    )[..., None]

    strip = jnp.asarray(kernel_strip(lag_count))
    size = width + width // 2 + 128
    words = pl.pallas_call(
        functools.partial(stack_kernel, lag_count),
        grid=(groups // 2,),
        in_specs=[
            pl.BlockSpec((days, None, owned, width), lambda g: (0, g, 0, 0)),
            pl.BlockSpec((days, None, owned, width), lambda g: (0, g, 0, 0)),
            pl.BlockSpec((2 * days, None, owned, 1), lambda g: (0, g, 0, 0)),
            pl.BlockSpec(strip.shape, lambda g: (0, 0)),
        ],
        out_specs=pl.BlockSpec((1, owned, size), lambda g: (g, 0, 0)),
        out_shape=jax.ShapeDtypeStruct((groups // 2, owned, size), jnp.int32),
        scratch_shapes=[
            pltpu.VMEM((width, width), jnp.bfloat16),
            pltpu.VMEM((2 * days * owned, width), jnp.bfloat16),
            pltpu.VMEM((3, owned, width), jnp.float32),
        ],
        compiler_params=pltpu.CompilerParams(vmem_limit_bytes=60 * 2**20),
        cost_estimate=pl.CostEstimate(
            flops=2 * days * pairs * width * width, bytes_accessed=days * pairs * width * 2, transcendentals=0
        ),
        name="stack",
    )(mine, other, scale, strip)

    same = [[c + 2 * i for i in range(groups // 2)] for c in range(2)]
    words = lax.all_to_all(words, "day", split_axis=0, concat_axis=0, axis_index_groups=same, tiled=True)

    out = jax.ShapeDtypeStruct((owned, lag_count), jnp.float32)
    return pl.pallas_call(
        functools.partial(finish_kernel, lag_count),
        out_shape=(out, out),
        compiler_params=pltpu.CompilerParams(vmem_limit_bytes=60 * 2**20),
        name="finish",
    )(words, counts[:, None])


def solution(mesh):
    placed = (P("day", "pair", None), P("day", "pair"), P(("pair", "day")))
    return jax.shard_map(
        shards,
        mesh=mesh,
        in_specs=placed,
        out_specs=(P(("pair", "day"), None), P(("pair", "day"), None)),
        check_vma=False,
    )
```

```python
import functools

import jax
import jax.numpy as jnp
import numpy as np
from jax import lax
from jax.experimental import pallas as pl
from jax.experimental.pallas import tpu as pltpu
from jax.sharding import PartitionSpec as P

TILE = 256
MESH = pl.DeviceIdType.MESH
FULL = 32767.0
UNIT = 2.0**20


def padded(lag_count):
    return -(-lag_count // TILE) * TILE


def kernel_strip(lag_count):
    f32 = np.float32
    offset = np.arange(lag_count, dtype=np.int32)
    offset = np.where(offset > lag_count // 2, offset - lag_count, offset)
    angle = f32(np.pi) * offset.astype(f32) / f32(lag_count)
    parity = f32(1) - f32(2) * (offset % 2).astype(f32)
    sine = np.where(offset == 0, f32(1), np.sin(angle)).astype(f32)
    kernel = np.where(offset == 0, f32(0), (np.cos(angle) - parity) / (f32(lag_count) * sine))
    width = padded(lag_count)
    index = np.arange(2 * width - TILE)[None, :] - np.arange(TILE)[:, None] - (width - TILE)
    return kernel.astype(f32)[index % lag_count].astype(jnp.bfloat16)


def codes(values):
    top = jnp.max(jnp.abs(values), axis=1, keepdims=True)
    units = (top * UNIT).astype(jnp.int32) + 1
    step = FULL * UNIT / units.astype(jnp.float32)
    return jnp.round(values * step).astype(jnp.int32), units


def join(high, low):
    return high * 65536 + (low & 65535)


def split(word):
    low = ((word & 65535) ^ 32768) - 32768
    return word >> 16, low


def stack_kernel(
    lag_count, x_hbm, mask_ref, counts_ref, strip_hbm, weighted_ref, linear_ref,
    rows_ref, stage, strip, table, sums, day_weight, stat_out, stat_in, words_out, words_in,
    load_sem, stage_sem, strip_sem, swap_send, swap_recv, stat_send, stat_recv, word_send, word_recv,
):
    width = table.shape[1]
    half = width // 2
    chips, all_days, owned, _ = rows_ref.shape
    days = all_days // 2
    total = all_days * owned
    peers = stat_in.shape[0]
    me, plane = lax.axis_index("day"), lax.axis_index("pair")
    chip, core = me // 2, me % 2
    last = width - TILE

    def mine(g):
        return pltpu.make_async_copy(x_hbm.at[:, 2 * g + core], rows_ref.at[g, pl.ds(0, days)], load_sem.at[g])

    def staged(g):
        return pltpu.make_async_copy(x_hbm.at[:, 2 * g + 1 - core], stage.at[g], stage_sem.at[g])

    def swapped(g):
        return pltpu.make_async_remote_copy(
            stage.at[g], rows_ref.at[g, pl.ds(days, days)], swap_send.at[g], swap_recv.at[g],
            device_id={"day": me ^ 1, "pair": plane}, device_id_type=MESH,
        )

    def peer(o):
        rank = (2 * plane + core + o) % (peers + 1)
        return {"day": 2 * chip + rank % 2, "pair": rank // 2}

    def told(o):
        return pltpu.make_async_remote_copy(
            stat_out, stat_in.at[o - 1], stat_send.at[o - 1], stat_recv.at[o - 1],
            device_id=peer(o), device_id_type=MESH,
        )

    def owner(o):
        return {"day": 2 * (chip ^ o) + core, "pair": plane}

    def shipped(o):
        return pltpu.make_async_remote_copy(
            words_out.at[o - 1], words_in.at[o - 1], word_send.at[o - 1], word_recv.at[o - 1],
            device_id=owner(o), device_id_type=MESH,
        )

    for g in range(chips):
        staged(g).start()
    for g in range(chips):
        mine(g).start()
    strip_copy = pltpu.make_async_copy(strip_hbm, strip, strip_sem)
    strip_copy.start()

    barrier = pltpu.get_barrier_semaphore()
    for o in range(1, peers + 1):
        pl.semaphore_signal(barrier, inc=1, device_id=peer(o), device_id_type=MESH)
    for o in range(1, chips):
        pl.semaphore_signal(barrier, inc=1, device_id=owner(o), device_id_type=MESH)
    pl.semaphore_wait(barrier, peers + chips - 1)

    for g in range(chips):
        staged(g).wait()
        swapped(g).start()

    def statistics(g, carry):
        mine(g).wait()
        swapped(g).wait_recv()
        x = rows_ref[g].reshape(total, lag_count).astype(jnp.float32)
        row_mask = mask_ref[g]
        energy = jnp.sum(x * x, axis=1, keepdims=True) * row_mask
        both = jnp.concatenate(
            [jnp.broadcast_to(energy, (total, 128)), jnp.broadcast_to(row_mask, (total, 128))], axis=1
        )
        return carry + jnp.sum(both.reshape(all_days, owned, 256), axis=1)

    found = lax.fori_loop(0, chips, statistics, jnp.zeros((all_days, 256), jnp.float32))
    turned = jnp.concatenate([found[days:], found[:days]], axis=0)
    stat_out[...] = jnp.where(core == 0, found, turned)
    for o in range(1, peers + 1):
        told(o).start()

    strip_copy.wait()
    for i in range(width // TILE):
        start = width - TILE - i * TILE
        table[pl.ds(i * TILE, TILE), :] = strip[:, start : start + width]
    sums[:, :, last:] = jnp.zeros((3, owned, TILE), jnp.float32)

    for o in range(1, peers + 1):
        told(o).wait_recv()
    stats = stat_out[...]
    for o in range(peers):
        stats = stats + stat_in[o]
    weight = lax.rsqrt(stats[:, :128] / (lag_count * jnp.maximum(stats[:, 128:], 1.0)) + 0.1)
    weight = jnp.where(core == 0, weight, jnp.concatenate([weight[days:], weight[:days]], axis=0))
    for d in range(all_days):
        day_weight[pl.ds(d * owned, owned), :] = jnp.broadcast_to(weight[d : d + 1, :1], (owned, 1))

    def block(step, carry):
        o = chips - 1 - step
        g = chip ^ o
        scale = day_weight[...] * mask_ref[g]
        for j in range(width // TILE):
            cols = slice(j * TILE, min((j + 1) * TILE, lag_count))
            size = cols.stop - cols.start
            lhs = rows_ref[g].reshape(total, lag_count)
            hilbert = jnp.dot(lhs, table[:lag_count, cols], preferred_element_type=jnp.float32)
            real = scale * rows_ref[g, :, :, cols].reshape(total, size).astype(jnp.float32)
            imag = scale * hilbert
            inverse = lax.rsqrt(real * real + imag * imag + 0.25)
            for k, term in enumerate((real, real * inverse, imag * inverse)):
                sums[k, :, cols] = jnp.sum(term.reshape(all_days, owned, size), axis=0)

        @pl.when(o > 0)
        def _():
            linear, linear_units = codes(sums[0])
            first, first_units = codes(sums[1])
            second, second_units = codes(sums[2])
            words_out[o - 1, :, :width] = join(first, second)
            words_out[o - 1, :, width : width + half] = join(linear[:, :half], linear[:, half:])
            pick = lax.broadcasted_iota(jnp.int32, (owned, 128), 1)
            words_out[o - 1, :, width + half :] = jnp.where(
                pick == 0, linear_units, jnp.where(pick == 1, first_units, second_units)
            )
            shipped(o).start()

        return carry

    lax.fori_loop(0, chips, block, 0)

    def arrive(step, carry):
        o = chips - 1 - step
        shipped(o).wait_recv()
        units = words_in[o - 1, :, width + half :].astype(jnp.float32) * (1.0 / (FULL * UNIT))
        left, right = split(words_in[o - 1, :, width : width + half])
        sums[0, :, :half] += left.astype(jnp.float32) * units[:, 0:1]
        sums[0, :, half:] += right.astype(jnp.float32) * units[:, 0:1]
        first, second = split(words_in[o - 1, :, :width])
        sums[1] += first.astype(jnp.float32) * units[:, 1:2]
        sums[2] += second.astype(jnp.float32) * units[:, 2:3]
        return carry

    lax.fori_loop(0, chips - 1, arrive, 0)
    inverse = 1.0 / jnp.maximum(counts_ref[...].astype(jnp.float32), 1.0)
    linear = sums[0, :, :lag_count] * inverse
    real, imag = sums[1, :, :lag_count], sums[2, :, :lag_count]
    linear_ref[...] = linear
    weighted_ref[...] = linear * ((real * real + imag * imag) * (inverse * inverse))

    for g in range(chips):
        swapped(g).wait_send()
    for o in range(1, peers + 1):
        told(o).wait_send()
    for o in range(1, chips):
        shipped(o).wait_send()


def shards(correlations, mask, counts):
    days, pairs, lag_count = correlations.shape
    groups = lax.axis_size("day")
    chips = groups // 2
    core = lax.axis_index("day") % 2
    owned = pairs // groups
    width = padded(lag_count)
    peers = 2 * lax.axis_size("pair") - 1

    mask_blocks = mask.astype(jnp.float32).reshape(days, chips, 2, owned)
    mask_mine, mask_other = (jnp.where(core == 0, mask_blocks[:, :, s], mask_blocks[:, :, 1 - s]) for s in (0, 1))
    mask_other = lax.ppermute(mask_other, "day", [(i, i ^ 1) for i in range(groups)])
    row_mask = jnp.concatenate([mask_mine, mask_other], axis=0).transpose(1, 0, 2)
    row_mask = row_mask.reshape(chips, 2 * days * owned, 1)

    strip = jnp.asarray(kernel_strip(lag_count))
    size = width + width // 2 + 128
    out = jax.ShapeDtypeStruct((owned, lag_count), jnp.float32)
    vmem = pl.BlockSpec(memory_space=pltpu.VMEM)
    hbm = pl.BlockSpec(memory_space=pl.ANY)
    dma = pltpu.SemaphoreType.DMA
    return pl.pallas_call(
        functools.partial(stack_kernel, lag_count),
        in_specs=[hbm, vmem, vmem, hbm],
        out_specs=(vmem, vmem),
        out_shape=(out, out),
        scratch_shapes=[
            pltpu.VMEM((chips, 2 * days, owned, lag_count), jnp.bfloat16),
            pltpu.VMEM((chips, days, owned, lag_count), jnp.bfloat16),
            pltpu.VMEM(strip.shape, jnp.bfloat16),
            pltpu.VMEM((width, width), jnp.bfloat16),
            pltpu.VMEM((3, owned, width), jnp.float32),
            pltpu.VMEM((2 * days * owned, 1), jnp.float32),
            pltpu.VMEM((2 * days, 256), jnp.float32),
            pltpu.VMEM((peers, 2 * days, 256), jnp.float32),
            pltpu.VMEM((chips - 1, owned, size), jnp.int32),
            pltpu.VMEM((chips - 1, owned, size), jnp.int32),
            dma((chips,)), dma((chips,)), dma, dma((chips,)), dma((chips,)),
            dma((peers,)), dma((peers,)), dma((chips - 1,)), dma((chips - 1,)),
        ],
        compiler_params=pltpu.CompilerParams(
            vmem_limit_bytes=62 * 2**20, collective_id=0, has_side_effects=True
        ),
        name="stack",
    )(correlations.reshape(days, groups, owned, lag_count), row_mask, counts[:, None], strip)


def solution(mesh):
    placed = (P("day", "pair", None), P("day", "pair"), P(("pair", "day")))
    return jax.shard_map(
        shards,
        mesh=mesh,
        in_specs=placed,
        out_specs=(P(("pair", "day"), None), P(("pair", "day"), None)),
        check_vma=False,
    )
```

```python
import functools

import jax
import jax.numpy as jnp
import numpy as np
from jax import lax
from jax.experimental import pallas as pl
from jax.experimental.pallas import tpu as pltpu
from jax.sharding import PartitionSpec as P

TILE = 256
MESH = pl.DeviceIdType.MESH
FULL = 32767.0
UNIT = 2.0**20


def padded(lag_count):
    return -(-lag_count // TILE) * TILE


def kernel_strip(lag_count):
    f32 = np.float32
    offset = np.arange(lag_count, dtype=np.int32)
    offset = np.where(offset > lag_count // 2, offset - lag_count, offset)
    angle = f32(np.pi) * offset.astype(f32) / f32(lag_count)
    parity = f32(1) - f32(2) * (offset % 2).astype(f32)
    sine = np.where(offset == 0, f32(1), np.sin(angle)).astype(f32)
    kernel = np.where(offset == 0, f32(0), (np.cos(angle) - parity) / (f32(lag_count) * sine))
    width = padded(lag_count)
    index = np.arange(2 * width - TILE)[None, :] - np.arange(TILE)[:, None] - (width - TILE)
    return kernel.astype(f32)[index % lag_count].astype(jnp.bfloat16)


def codes(values):
    top = jnp.max(jnp.abs(values), axis=1, keepdims=True)
    units = (top * UNIT).astype(jnp.int32) + 1
    step = FULL * UNIT / units.astype(jnp.float32)
    return jnp.round(values * step).astype(jnp.int32), units


def join(high, low):
    return high * 65536 + (low & 65535)


def split(word):
    low = ((word & 65535) ^ 32768) - 32768
    return word >> 16, low


def stack_kernel(
    lag_count, x_hbm, mask_ref, strip_hbm, linear_ref, power_ref,
    rows_ref, stage, strip, table, sums, first_hilbert, mask_in, mask_turned, row_mask, day_weight,
    stat_out, stat_in, words_out, words_in,
    load_sem, stage_sem, strip_sem, swap_send, swap_recv, mask_send, mask_recv,
    stat_send, stat_recv, word_send, word_recv,
):
    width = table.shape[1]
    half = width // 2
    chips, all_days, owned, _ = rows_ref.shape
    days = all_days // 2
    total = all_days * owned
    peers = stat_in.shape[0]
    me, plane = lax.axis_index("day"), lax.axis_index("pair")
    chip, core = me // 2, me % 2
    partner = {"day": me ^ 1, "pair": plane}
    last = width - TILE
    tiles = [slice(j * TILE, min((j + 1) * TILE, lag_count)) for j in range(width // TILE)]

    def mine(g):
        return pltpu.make_async_copy(x_hbm.at[:, 2 * g + core], rows_ref.at[g, pl.ds(0, days)], load_sem.at[g])

    def staged(g):
        return pltpu.make_async_copy(x_hbm.at[:, 2 * g + 1 - core], stage.at[g], stage_sem.at[g])

    def swapped(g):
        return pltpu.make_async_remote_copy(
            stage.at[g], rows_ref.at[g, pl.ds(days, days)], swap_send.at[g], swap_recv.at[g],
            device_id=partner, device_id_type=MESH,
        )

    def peer(o):
        rank = (2 * plane + core + o) % (peers + 1)
        return {"day": 2 * chip + rank % 2, "pair": rank // 2}

    def told(o):
        return pltpu.make_async_remote_copy(
            stat_out, stat_in.at[o - 1], stat_send.at[o - 1], stat_recv.at[o - 1],
            device_id=peer(o), device_id_type=MESH,
        )

    def owner(o):
        return {"day": 2 * (chip ^ o) + core, "pair": plane}

    def shipped(o):
        return pltpu.make_async_remote_copy(
            words_out.at[o - 1], words_in.at[o - 1], word_send.at[o - 1], word_recv.at[o - 1],
            device_id=owner(o), device_id_type=MESH,
        )

    order = [chip ^ o for o in range(chips - 1, -1, -1)]
    for g in order:
        staged(g).start()
        mine(g).start()
    strip_copy = pltpu.make_async_copy(strip_hbm, strip, strip_sem)
    strip_copy.start()

    barrier = pltpu.get_barrier_semaphore()
    for o in range(1, peers + 1):
        pl.semaphore_signal(barrier, inc=1, device_id=peer(o), device_id_type=MESH)
    for o in range(1, chips):
        pl.semaphore_signal(barrier, inc=1, device_id=owner(o), device_id_type=MESH)
    pl.semaphore_wait(barrier, peers + chips - 1)

    mask_copy = pltpu.make_async_remote_copy(
        mask_ref, mask_in, mask_send, mask_recv, device_id=partner, device_id_type=MESH
    )
    mask_copy.start()
    for g in order:
        staged(g).wait()
        swapped(g).start()
    mask_copy.wait_recv()
    both_masks = jnp.concatenate([mask_ref[...], mask_in[...]], axis=0).astype(jnp.float32)
    mask_turned[...] = both_masks.T

    def mask_rows(block, count):
        rows = mask_turned[pl.ds(pl.multiple_of(block * owned, owned), owned), :]
        return jnp.concatenate([rows[:, d : d + 1] for d in range(count)], axis=0)

    def statistics(step, carry):
        g = chip ^ (chips - 1 - step)
        mine(g).wait()
        row_mask[g] = mask_rows(2 * g + core, all_days)
        for x_ref, rows in ((rows_ref.at[g, pl.ds(0, days)], row_mask[g, : days * owned]),
                            (stage.at[g], mask_rows(2 * g + 1 - core, days))):
            x = x_ref[...].reshape(days * owned, lag_count).astype(jnp.float32)
            energy = jnp.sum(x * x, axis=1, keepdims=True) * rows
            both = jnp.concatenate(
                [jnp.broadcast_to(energy, (days * owned, 128)), jnp.broadcast_to(rows, (days * owned, 128))], axis=1
            )
            carry = carry + jnp.sum(both.reshape(days, owned, 256), axis=1)
        return carry

    found = lax.fori_loop(0, chips, statistics, jnp.zeros((days, 256), jnp.float32))
    none = jnp.zeros_like(found)
    stat_out[...] = jnp.where(
        core == 0, jnp.concatenate([found, none], axis=0), jnp.concatenate([none, found], axis=0)
    )
    for o in range(1, peers + 1):
        told(o).start()

    strip_copy.wait()
    for i in range(width // TILE):
        start = width - TILE - i * TILE
        table[pl.ds(i * TILE, TILE), :] = strip[:, start : start + width]
    sums[:, :, last:] = jnp.zeros((3, owned, TILE), jnp.float32)

    def transform(g, cols):
        lhs = rows_ref[g].reshape(total, lag_count)
        return jnp.dot(lhs, table[:lag_count, cols], preferred_element_type=jnp.float32)

    def add_days(g, scale, cols, hilbert):
        size = cols.stop - cols.start
        real = scale * rows_ref[g, :, :, cols].reshape(total, size).astype(jnp.float32)
        imag = scale * hilbert
        inverse = lax.rsqrt(real * real + imag * imag + 0.25)
        for k, term in enumerate((real, real * inverse, imag * inverse)):
            sums[k, :, cols] = jnp.sum(term.reshape(all_days, owned, size), axis=0)

    def encode(o):
        linear, linear_units = codes(sums[0])
        first, first_units = codes(sums[1])
        second, second_units = codes(sums[2])
        words_out[o - 1, :, :width] = join(first, second)
        words_out[o - 1, :, width : width + half] = join(linear[:, :half], linear[:, half:])
        pick = lax.broadcasted_iota(jnp.int32, (owned, 128), 1)
        words_out[o - 1, :, width + half :] = jnp.where(
            pick == 0, linear_units, jnp.where(pick == 1, first_units, second_units)
        )
        shipped(o).start()

    swapped(order[0]).wait_recv()
    for cols in tiles:
        first_hilbert[:, cols] = transform(order[0], cols)

    for o in range(1, peers + 1):
        told(o).wait_recv()
    stats = stat_out[...]
    for o in range(peers):
        stats = stats + stat_in[o]
    weight = lax.rsqrt(stats[:, :128] / (lag_count * jnp.maximum(stats[:, 128:], 1.0)) + 0.1)
    weight = jnp.where(core == 0, weight, jnp.concatenate([weight[days:], weight[:days]], axis=0))
    for d in range(all_days):
        day_weight[pl.ds(d * owned, owned), :] = jnp.broadcast_to(weight[d : d + 1, :1], (owned, 1))

    scale = day_weight[...] * row_mask[order[0]]
    for cols in tiles:
        add_days(order[0], scale, cols, first_hilbert[:, cols])
    encode(chips - 1)

    def block(step, carry):
        o = chips - 1 - step
        g = chip ^ o
        swapped(g).wait_recv()
        scale = day_weight[...] * row_mask[g]
        for cols in tiles:
            add_days(g, scale, cols, transform(g, cols))

        @pl.when(o > 0)
        def _():
            encode(o)

        return carry

    lax.fori_loop(1, chips, block, 0)

    def arrive(step, carry):
        o = chips - 1 - step
        shipped(o).wait_recv()
        units = words_in[o - 1, :, width + half :].astype(jnp.float32) * (1.0 / (FULL * UNIT))
        left, right = split(words_in[o - 1, :, width : width + half])
        sums[0, :, :half] += left.astype(jnp.float32) * units[:, 0:1]
        sums[0, :, half:] += right.astype(jnp.float32) * units[:, 0:1]
        first, second = split(words_in[o - 1, :, :width])
        sums[1] += first.astype(jnp.float32) * units[:, 1:2]
        sums[2] += second.astype(jnp.float32) * units[:, 2:3]
        return carry

    lax.fori_loop(0, chips - 1, arrive, 0)
    real, imag = sums[1, :, :lag_count], sums[2, :, :lag_count]
    linear_ref[...] = sums[0, :, :lag_count]
    power_ref[...] = real * real + imag * imag

    mask_copy.wait_send()
    for g in range(chips):
        swapped(g).wait_send()
    for o in range(1, peers + 1):
        told(o).wait_send()
    for o in range(1, chips):
        shipped(o).wait_send()


def shards(correlations, mask, counts):
    days, pairs, lag_count = correlations.shape
    groups = lax.axis_size("day")
    chips = groups // 2
    owned = pairs // groups
    width = padded(lag_count)
    peers = 2 * lax.axis_size("pair") - 1

    strip = jnp.asarray(kernel_strip(lag_count))
    size = width + width // 2 + 128
    out = jax.ShapeDtypeStruct((owned, lag_count), jnp.float32)
    vmem = pl.BlockSpec(memory_space=pltpu.VMEM)
    hbm = pl.BlockSpec(memory_space=pl.ANY)
    dma = pltpu.SemaphoreType.DMA
    linear_sum, power = pl.pallas_call(
        functools.partial(stack_kernel, lag_count),
        in_specs=[hbm, vmem, hbm],
        out_specs=(vmem, vmem),
        out_shape=(out, out),
        scratch_shapes=[
            pltpu.VMEM((chips, 2 * days, owned, lag_count), jnp.bfloat16),
            pltpu.VMEM((chips, days, owned, lag_count), jnp.bfloat16),
            pltpu.VMEM(strip.shape, jnp.bfloat16),
            pltpu.VMEM((width, width), jnp.bfloat16),
            pltpu.VMEM((3, owned, width), jnp.float32),
            pltpu.VMEM((2 * days * owned, width), jnp.float32),
            pltpu.VMEM((days, pairs), jnp.int32),
            pltpu.VMEM((pairs, 2 * days), jnp.float32),
            pltpu.VMEM((chips, 2 * days * owned, 1), jnp.float32),
            pltpu.VMEM((2 * days * owned, 1), jnp.float32),
            pltpu.VMEM((2 * days, 256), jnp.float32),
            pltpu.VMEM((peers, 2 * days, 256), jnp.float32),
            pltpu.VMEM((chips - 1, owned, size), jnp.int32),
            pltpu.VMEM((chips - 1, owned, size), jnp.int32),
            dma((chips,)), dma((chips,)), dma, dma((chips,)), dma((chips,)), dma, dma,
            dma((peers,)), dma((peers,)), dma((chips - 1,)), dma((chips - 1,)),
        ],
        compiler_params=pltpu.CompilerParams(
            vmem_limit_bytes=62 * 2**20, collective_id=0, has_side_effects=True
        ),
        name="stack",
    )(correlations.reshape(days, groups, owned, lag_count), mask, strip)
    divisor = jnp.maximum(counts.astype(jnp.float32), 1.0)[:, None]
    linear = linear_sum / divisor
    return (linear * (power / (divisor * divisor)), linear)


def solution(mesh):
    placed = (P("day", "pair", None), P("day", "pair"), P(("pair", "day")))
    return jax.shard_map(
        shards,
        mesh=mesh,
        in_specs=placed,
        out_specs=(P(("pair", "day"), None), P(("pair", "day"), None)),
        check_vma=False,
    )
```

```python
import functools

import jax
import jax.numpy as jnp
import numpy as np
from jax import lax
from jax.experimental import pallas as pl
from jax.experimental.pallas import tpu as pltpu
from jax.sharding import PartitionSpec as P

TILE = 256
MESH = pl.DeviceIdType.MESH
FULL = 32767.0
UNIT = 2.0**20


def padded(lag_count):
    return -(-lag_count // TILE) * TILE


def kernel_strip(lag_count):
    f32 = np.float32
    offset = np.arange(lag_count, dtype=np.int32)
    offset = np.where(offset > lag_count // 2, offset - lag_count, offset)
    angle = f32(np.pi) * offset.astype(f32) / f32(lag_count)
    parity = f32(1) - f32(2) * (offset % 2).astype(f32)
    sine = np.where(offset == 0, f32(1), np.sin(angle)).astype(f32)
    kernel = np.where(offset == 0, f32(0), (np.cos(angle) - parity) / (f32(lag_count) * sine))
    width = padded(lag_count)
    index = np.arange(2 * width - TILE)[None, :] - np.arange(TILE)[:, None] - (width - TILE)
    return kernel.astype(f32)[index % lag_count].astype(jnp.bfloat16)


def codes(values):
    top = jnp.max(jnp.abs(values), axis=1, keepdims=True)
    units = (top * UNIT).astype(jnp.int32) + 1
    step = FULL * UNIT / units.astype(jnp.float32)
    return jnp.round(values * step).astype(jnp.int32), units


def join(high, low):
    return high * 65536 + (low & 65535)


def split(word):
    low = ((word & 65535) ^ 32768) - 32768
    return word >> 16, low


def stack_kernel(
    lag_count, x_hbm, mask_ref, strip_hbm, linear_ref, power_ref,
    rows_ref, stage, strip, table, sums, first_hilbert, mask_in, mask_turned, row_mask, day_weight,
    stat_out, stat_in, words_out, words_in,
    load_sem, stage_sem, strip_sem, swap_send, swap_recv, mask_send, mask_recv,
    stat_send, stat_recv, word_send, word_recv,
):
    width = table.shape[1]
    half = width // 2
    chips, all_days, owned, _ = rows_ref.shape
    days = all_days // 2
    total = all_days * owned
    part = owned // 2
    pieces = words_out.shape[0]
    peers = stat_in.shape[0]
    me, plane = lax.axis_index("day"), lax.axis_index("pair")
    chip, core = me // 2, me % 2
    partner = {"day": me ^ 1, "pair": plane}
    last = width - TILE
    tiles = [slice(j * TILE, min((j + 1) * TILE, lag_count)) for j in range(width // TILE)]

    def mine(g):
        return pltpu.make_async_copy(x_hbm.at[:, 2 * g + core], rows_ref.at[g, pl.ds(0, days)], load_sem.at[g])

    def staged(g):
        return pltpu.make_async_copy(x_hbm.at[:, 2 * g + 1 - core], stage.at[g], stage_sem.at[g])

    def swapped(g):
        return pltpu.make_async_remote_copy(
            stage.at[g], rows_ref.at[g, pl.ds(days, days)], swap_send.at[g], swap_recv.at[g],
            device_id=partner, device_id_type=MESH,
        )

    def peer(o):
        rank = (2 * plane + core + o) % (peers + 1)
        return {"day": 2 * chip + rank % 2, "pair": rank // 2}

    def told(o):
        return pltpu.make_async_remote_copy(
            stat_out, stat_in.at[o - 1], stat_send.at[o - 1], stat_recv.at[o - 1],
            device_id=peer(o), device_id_type=MESH,
        )

    def owner(o):
        return {"day": 2 * (chip ^ o) + core, "pair": plane}

    def shipped(piece, o):
        return pltpu.make_async_remote_copy(
            words_out.at[piece], words_in.at[piece], word_send.at[piece], word_recv.at[piece],
            device_id=owner(o), device_id_type=MESH,
        )

    far = range(chips - 1, 3, -1)
    order = [chip ^ o for o in (3, *far, 1, 2, 0)]
    for g in order:
        staged(g).start()
        mine(g).start()
    strip_copy = pltpu.make_async_copy(strip_hbm, strip, strip_sem)
    strip_copy.start()

    barrier = pltpu.get_barrier_semaphore()
    for o in range(1, peers + 1):
        pl.semaphore_signal(barrier, inc=1, device_id=peer(o), device_id_type=MESH)
    for o in range(1, chips):
        pl.semaphore_signal(barrier, inc=1, device_id=owner(o), device_id_type=MESH)
    pl.semaphore_wait(barrier, peers + chips - 1)

    mask_copy = pltpu.make_async_remote_copy(
        mask_ref, mask_in, mask_send, mask_recv, device_id=partner, device_id_type=MESH
    )
    mask_copy.start()
    for g in order:
        staged(g).wait()
        swapped(g).start()
    mask_copy.wait_recv()
    both_masks = jnp.concatenate([mask_ref[...], mask_in[...]], axis=0).astype(jnp.float32)
    mask_turned[...] = both_masks.T

    def mask_rows(block, count):
        rows = mask_turned[pl.ds(pl.multiple_of(block * owned, owned), owned), :]
        return jnp.concatenate([rows[:, d : d + 1] for d in range(count)], axis=0)

    def statistics(step, carry):
        g = chip ^ (chips - 1 - step)
        mine(g).wait()
        of_pairs = mask_rows(2 * g + core, all_days)
        row_mask[g] = of_pairs.reshape(all_days, owned, 1)
        for x_ref, rows in ((rows_ref.at[g, pl.ds(0, days)], of_pairs[: days * owned]),
                            (stage.at[g], mask_rows(2 * g + 1 - core, days))):
            x = x_ref[...].reshape(days * owned, lag_count).astype(jnp.float32)
            energy = jnp.sum(x * x, axis=1, keepdims=True) * rows
            both = jnp.concatenate(
                [jnp.broadcast_to(energy, (days * owned, 128)), jnp.broadcast_to(rows, (days * owned, 128))], axis=1
            )
            carry = carry + jnp.sum(both.reshape(days, owned, 256), axis=1)
        return carry

    found = lax.fori_loop(0, chips, statistics, jnp.zeros((days, 256), jnp.float32))
    none = jnp.zeros_like(found)
    stat_out[...] = jnp.where(
        core == 0, jnp.concatenate([found, none], axis=0), jnp.concatenate([none, found], axis=0)
    )
    for o in range(1, peers + 1):
        told(o).start()

    strip_copy.wait()
    for i in range(width // TILE):
        start = width - TILE - i * TILE
        table[pl.ds(i * TILE, TILE), :] = strip[:, start : start + width]
    sums[:, :, last:] = jnp.zeros((3, owned, TILE), jnp.float32)

    def transform(g, here, cols):
        lhs = rows_ref[g, :, here, :].reshape(-1, lag_count)
        return jnp.dot(lhs, table[:lag_count, cols], preferred_element_type=jnp.float32)

    def add_days(g, here, cols, hilbert):
        size = cols.stop - cols.start
        count = hilbert.shape[0] // all_days
        scale = (day_weight[:, :count] * row_mask[g, :, here, :]).reshape(-1, 1)
        real = scale * rows_ref[g, :, here, cols].reshape(-1, size).astype(jnp.float32)
        imag = scale * hilbert
        inverse = lax.rsqrt(real * real + imag * imag + 0.25)
        for k, term in enumerate((real, real * inverse, imag * inverse)):
            sums[k, :count, cols] = jnp.sum(term.reshape(all_days, count, size), axis=0)

    def encode(piece, rows, o):
        linear, linear_units = codes(sums[0, rows])
        first, first_units = codes(sums[1, rows])
        second, second_units = codes(sums[2, rows])
        words_out[piece, :, :width] = join(first, second)
        words_out[piece, :, width : width + half] = join(linear[:, :half], linear[:, half:])
        pick = lax.broadcasted_iota(jnp.int32, (part, 128), 1)
        words_out[piece, :, width + half :] = jnp.where(
            pick == 0, linear_units, jnp.where(pick == 1, first_units, second_units)
        )
        shipped(piece, o).start()

    def decode(piece, rows):
        units = words_in[piece, :, width + half :].astype(jnp.float32) * (1.0 / (FULL * UNIT))
        left, right = split(words_in[piece, :, width : width + half])
        sums[0, rows, :half] += left.astype(jnp.float32) * units[:, 0:1]
        sums[0, rows, half:] += right.astype(jnp.float32) * units[:, 0:1]
        first, second = split(words_in[piece, :, :width])
        sums[1, rows] += first.astype(jnp.float32) * units[:, 1:2]
        sums[2, rows] += second.astype(jnp.float32) * units[:, 2:3]

    whole, low, high = pl.ds(0, owned), pl.ds(0, part), pl.ds(part, part)

    swapped(order[0]).wait_recv()
    for cols in tiles:
        first_hilbert[:, cols] = transform(order[0], whole, cols)

    for o in range(1, peers + 1):
        told(o).wait_recv()
    stats = stat_out[...]
    for o in range(peers):
        stats = stats + stat_in[o]
    weight = lax.rsqrt(stats[:, :128] / (lag_count * jnp.maximum(stats[:, 128:], 1.0)) + 0.1)
    weight = jnp.where(core == 0, weight, jnp.concatenate([weight[days:], weight[:days]], axis=0))
    for d in range(all_days):
        day_weight[d] = jnp.broadcast_to(weight[d : d + 1, :1], (owned, 1))

    for cols in tiles:
        add_days(order[0], whole, cols, first_hilbert[:, cols])
    encode(0, low, 1)
    encode(1, high, 2)

    def far_block(step, carry):
        o = chips - 1 - step
        swapped(chip ^ o).wait_recv()
        for cols in tiles:
            add_days(chip ^ o, whole, cols, transform(chip ^ o, whole, cols))
        encode(2 * o - 2, low, o)
        encode(2 * o - 1, high, o)
        return carry

    if chips > 4:
        lax.fori_loop(0, chips - 4, far_block, 0)

    def near_half(q, carry):
        o = 1 + q % 2
        g = chip ^ o
        here = pl.ds(pl.multiple_of(((q + q // 2) % 2) * part, part), part)

        @pl.when(q < 2)
        def _():
            swapped(g).wait_recv()

        for cols in tiles:
            add_days(g, here, cols, transform(g, here, cols))

        @pl.when(q >= 2)
        def _():
            shipped(3 - q, o).wait_recv()
            decode(3 - q, low)

        encode(2 + q, low, o)
        return carry

    lax.fori_loop(0, 4, near_half, 0)
    swapped(chip).wait_recv()
    for cols in tiles:
        add_days(chip, whole, cols, transform(chip, whole, cols))

    def arrive(piece, carry):
        turn = piece + jnp.where(piece // 2 == 2, 1, 0)
        shipped(piece, 1).wait_recv()
        decode(piece, pl.ds(pl.multiple_of((turn % 2) * part, part), part))
        return carry

    lax.fori_loop(2, pieces, arrive, 0)
    real, imag = sums[1, :, :lag_count], sums[2, :, :lag_count]
    linear_ref[...] = sums[0, :, :lag_count]
    power_ref[...] = real * real + imag * imag

    mask_copy.wait_send()
    for g in range(chips):
        swapped(g).wait_send()
    for o in range(1, peers + 1):
        told(o).wait_send()
    for piece in range(pieces):
        shipped(piece, 1).wait_send()


def shards(correlations, mask, counts):
    days, pairs, lag_count = correlations.shape
    groups = lax.axis_size("day")
    chips = groups // 2
    owned = pairs // groups
    width = padded(lag_count)
    peers = 2 * lax.axis_size("pair") - 1

    strip = jnp.asarray(kernel_strip(lag_count))
    size = width + width // 2 + 128
    pieces = 2 * chips - 2
    out = jax.ShapeDtypeStruct((owned, lag_count), jnp.float32)
    vmem = pl.BlockSpec(memory_space=pltpu.VMEM)
    hbm = pl.BlockSpec(memory_space=pl.ANY)
    dma = pltpu.SemaphoreType.DMA
    linear_sum, power = pl.pallas_call(
        functools.partial(stack_kernel, lag_count),
        in_specs=[hbm, vmem, hbm],
        out_specs=(vmem, vmem),
        out_shape=(out, out),
        scratch_shapes=[
            pltpu.VMEM((chips, 2 * days, owned, lag_count), jnp.bfloat16),
            pltpu.VMEM((chips, days, owned, lag_count), jnp.bfloat16),
            pltpu.VMEM(strip.shape, jnp.bfloat16),
            pltpu.VMEM((width, width), jnp.bfloat16),
            pltpu.VMEM((3, owned, width), jnp.float32),
            pltpu.VMEM((2 * days * owned, width), jnp.float32),
            pltpu.VMEM((days, pairs), jnp.int32),
            pltpu.VMEM((pairs, 2 * days), jnp.float32),
            pltpu.VMEM((chips, 2 * days, owned, 1), jnp.float32),
            pltpu.VMEM((2 * days, owned, 1), jnp.float32),
            pltpu.VMEM((2 * days, 256), jnp.float32),
            pltpu.VMEM((peers, 2 * days, 256), jnp.float32),
            pltpu.VMEM((pieces, owned // 2, size), jnp.int32),
            pltpu.VMEM((pieces, owned // 2, size), jnp.int32),
            dma((chips,)), dma((chips,)), dma, dma((chips,)), dma((chips,)), dma, dma,
            dma((peers,)), dma((peers,)), dma((pieces,)), dma((pieces,)),
        ],
        compiler_params=pltpu.CompilerParams(
            vmem_limit_bytes=62 * 2**20, collective_id=0, has_side_effects=True
        ),
        name="stack",
    )(correlations.reshape(days, groups, owned, lag_count), mask, strip)
    divisor = jnp.maximum(counts.astype(jnp.float32), 1.0)[:, None]
    linear = linear_sum / divisor
    return (linear * (power / (divisor * divisor)), linear)


def solution(mesh):
    placed = (P("day", "pair", None), P("day", "pair"), P(("pair", "day")))
    return jax.shard_map(
        shards,
        mesh=mesh,
        in_specs=placed,
        out_specs=(P(("pair", "day"), None), P(("pair", "day"), None)),
        check_vma=False,
    )
```

```python
import functools

import jax
import jax.numpy as jnp
import numpy as np
from jax import lax
from jax.experimental import pallas as pl
from jax.experimental.pallas import tpu as pltpu
from jax.sharding import PartitionSpec as P

TILE = 256
MESH = pl.DeviceIdType.MESH
FULL = 32767.0
UNIT = 2.0**20


def padded(lag_count):
    return -(-lag_count // TILE) * TILE


def kernel_strip(lag_count):
    f32 = np.float32
    offset = np.arange(lag_count, dtype=np.int32)
    offset = np.where(offset > lag_count // 2, offset - lag_count, offset)
    angle = f32(np.pi) * offset.astype(f32) / f32(lag_count)
    parity = f32(1) - f32(2) * (offset % 2).astype(f32)
    sine = np.where(offset == 0, f32(1), np.sin(angle)).astype(f32)
    kernel = np.where(offset == 0, f32(0), (np.cos(angle) - parity) / (f32(lag_count) * sine))
    width = padded(lag_count)
    index = np.arange(2 * width - TILE)[None, :] - np.arange(TILE)[:, None] - (width - TILE)
    return kernel.astype(f32)[index % lag_count].astype(jnp.bfloat16)


def codes(values):
    top = jnp.max(jnp.abs(values), axis=1, keepdims=True)
    units = (top * UNIT).astype(jnp.int32) + 1
    step = FULL * UNIT / units.astype(jnp.float32)
    return jnp.round(values * step).astype(jnp.int32), units


def join(high, low):
    return high * 65536 + (low & 65535)


def split(word):
    low = ((word & 65535) ^ 32768) - 32768
    return word >> 16, low


def stack_kernel(
    lag_count, x_hbm, mask_ref, strip_hbm, linear_ref, power_ref,
    rows_ref, stage, strip, table, sums, first_hilbert, mask_in, mask_turned, row_mask, day_weight,
    stat_out, stat_in, words_out, words_in,
    load_sem, stage_sem, strip_sem, swap_send, swap_recv, mask_send, mask_recv,
    stat_send, stat_recv, word_send, word_recv,
):
    width = table.shape[1]
    half = width // 2
    chips, all_days, owned, _ = rows_ref.shape
    days = all_days // 2
    total = all_days * owned
    part = owned // 2
    pieces = words_out.shape[0]
    peers = stat_in.shape[0]
    me, plane = lax.axis_index("day"), lax.axis_index("pair")
    chip, core = me // 2, me % 2
    partner = {"day": me ^ 1, "pair": plane}
    last = width - TILE
    tiles = [slice(j * TILE, min((j + 1) * TILE, lag_count)) for j in range(width // TILE)]

    def mine(g):
        return pltpu.make_async_copy(x_hbm.at[:, 2 * g + core], rows_ref.at[g, pl.ds(0, days)], load_sem.at[g])

    def staged(g):
        return pltpu.make_async_copy(x_hbm.at[:, 2 * g + 1 - core], stage.at[g], stage_sem.at[g])

    def swapped(g):
        return pltpu.make_async_remote_copy(
            stage.at[g], rows_ref.at[g, pl.ds(days, days)], swap_send.at[g], swap_recv.at[g],
            device_id=partner, device_id_type=MESH,
        )

    def peer(o):
        rank = (2 * plane + core + o) % (peers + 1)
        return {"day": 2 * chip + rank % 2, "pair": rank // 2}

    def told(o):
        return pltpu.make_async_remote_copy(
            stat_out, stat_in.at[o - 1], stat_send.at[o - 1], stat_recv.at[o - 1],
            device_id=peer(o), device_id_type=MESH,
        )

    def owner(o):
        return {"day": 2 * (chip ^ o) + core, "pair": plane}

    def shipped(piece, o):
        return pltpu.make_async_remote_copy(
            words_out.at[piece], words_in.at[piece], word_send.at[piece], word_recv.at[piece],
            device_id=owner(o), device_id_type=MESH,
        )

    far = range(chips - 1, 3, -1)
    order = [chip ^ o for o in (3, *far, 1, 2, 0)]
    strip_copy = pltpu.make_async_copy(strip_hbm, strip, strip_sem)
    strip_copy.start()
    for g in order:
        staged(g).start()
        mine(g).start()

    barrier = pltpu.get_barrier_semaphore()
    for o in range(1, peers + 1):
        pl.semaphore_signal(barrier, inc=1, device_id=peer(o), device_id_type=MESH)
    for o in range(1, chips):
        pl.semaphore_signal(barrier, inc=1, device_id=owner(o), device_id_type=MESH)
    strip_copy.wait()
    for i in range(width // TILE):
        start = width - TILE - i * TILE
        table[pl.ds(i * TILE, TILE), :] = strip[:, start : start + width]
    sums[:, :, last:] = jnp.zeros((3, owned, TILE), jnp.float32)
    pl.semaphore_wait(barrier, peers + chips - 1)

    mask_copy = pltpu.make_async_remote_copy(
        mask_ref, mask_in, mask_send, mask_recv, device_id=partner, device_id_type=MESH
    )
    mask_copy.start()
    for g in order:
        staged(g).wait()
        swapped(g).start()
    mask_copy.wait_recv()
    both_masks = jnp.concatenate([mask_ref[...], mask_in[...]], axis=0).astype(jnp.float32)
    mask_turned[...] = both_masks.T

    def mask_rows(block, count):
        rows = mask_turned[pl.ds(pl.multiple_of(block * owned, owned), owned), :]
        return jnp.concatenate([rows[:, d : d + 1] for d in range(count)], axis=0)

    def statistics(step, carry):
        g = chip ^ (chips - 1 - step)
        mine(g).wait()
        of_pairs = mask_rows(2 * g + core, all_days)
        row_mask[g] = of_pairs.reshape(all_days, owned, 1)
        for x_ref, rows in ((rows_ref.at[g, pl.ds(0, days)], of_pairs[: days * owned]),
                            (stage.at[g], mask_rows(2 * g + 1 - core, days))):
            x = x_ref[...].reshape(days * owned, lag_count).astype(jnp.float32)
            energy = jnp.sum(x * x, axis=1, keepdims=True) * rows
            both = jnp.concatenate(
                [jnp.broadcast_to(energy, (days * owned, 128)), jnp.broadcast_to(rows, (days * owned, 128))], axis=1
            )
            carry = carry + jnp.sum(both.reshape(days, owned, 256), axis=1)
        return carry

    found = lax.fori_loop(0, chips, statistics, jnp.zeros((days, 256), jnp.float32))
    none = jnp.zeros_like(found)
    stat_out[...] = jnp.where(
        core == 0, jnp.concatenate([found, none], axis=0), jnp.concatenate([none, found], axis=0)
    )
    for o in range(1, peers + 1):
        told(o).start()

    def transform(g, here, cols):
        lhs = rows_ref[g, :, here, :].reshape(-1, lag_count)
        return jnp.dot(lhs, table[:lag_count, cols], preferred_element_type=jnp.float32)

    def add_days(g, here, cols, hilbert):
        size = cols.stop - cols.start
        count = hilbert.shape[0] // all_days
        scale = (day_weight[:, :count] * row_mask[g, :, here, :]).reshape(-1, 1)
        real = scale * rows_ref[g, :, here, cols].reshape(-1, size).astype(jnp.float32)
        imag = scale * hilbert
        inverse = lax.rsqrt(real * real + imag * imag + 0.25)
        for k, term in enumerate((real, real * inverse, imag * inverse)):
            sums[k, :count, cols] = jnp.sum(term.reshape(all_days, count, size), axis=0)

    def encode(piece, rows, o):
        linear, linear_units = codes(sums[0, rows])
        first, first_units = codes(sums[1, rows])
        second, second_units = codes(sums[2, rows])
        words_out[piece, :, :width] = join(first, second)
        words_out[piece, :, width : width + half] = join(linear[:, :half], linear[:, half:])
        pick = lax.broadcasted_iota(jnp.int32, (part, 128), 1)
        words_out[piece, :, width + half :] = jnp.where(
            pick == 0, linear_units, jnp.where(pick == 1, first_units, second_units)
        )
        shipped(piece, o).start()

    def decode(piece, rows):
        units = words_in[piece, :, width + half :].astype(jnp.float32) * (1.0 / (FULL * UNIT))
        left, right = split(words_in[piece, :, width : width + half])
        sums[0, rows, :half] += left.astype(jnp.float32) * units[:, 0:1]
        sums[0, rows, half:] += right.astype(jnp.float32) * units[:, 0:1]
        first, second = split(words_in[piece, :, :width])
        sums[1, rows] += first.astype(jnp.float32) * units[:, 1:2]
        sums[2, rows] += second.astype(jnp.float32) * units[:, 2:3]

    whole, low, high = pl.ds(0, owned), pl.ds(0, part), pl.ds(part, part)

    swapped(order[0]).wait_recv()
    for cols in tiles:
        first_hilbert[:, cols] = transform(order[0], whole, cols)

    for o in range(1, peers + 1):
        told(o).wait_recv()
    stats = stat_out[...]
    for o in range(peers):
        stats = stats + stat_in[o]
    weight = lax.rsqrt(stats[:, :128] / (lag_count * jnp.maximum(stats[:, 128:], 1.0)) + 0.1)
    weight = jnp.where(core == 0, weight, jnp.concatenate([weight[days:], weight[:days]], axis=0))
    for d in range(all_days):
        day_weight[d] = jnp.broadcast_to(weight[d : d + 1, :1], (owned, 1))

    for cols in tiles:
        add_days(order[0], whole, cols, first_hilbert[:, cols])
    encode(0, low, 1)
    encode(1, high, 2)

    def far_block(step, carry):
        o = chips - 1 - step
        swapped(chip ^ o).wait_recv()
        for cols in tiles:
            add_days(chip ^ o, whole, cols, transform(chip ^ o, whole, cols))
        encode(2 * o - 2, low, o)
        encode(2 * o - 1, high, o)
        return carry

    if chips > 4:
        lax.fori_loop(0, chips - 4, far_block, 0)

    def near_half(q, carry):
        o = 1 + q % 2
        g = chip ^ o
        here = pl.ds(pl.multiple_of(((q + q // 2) % 2) * part, part), part)

        @pl.when(q < 2)
        def _():
            swapped(g).wait_recv()

        for cols in tiles:
            add_days(g, here, cols, transform(g, here, cols))

        @pl.when(q >= 2)
        def _():
            shipped(3 - q, o).wait_recv()
            decode(3 - q, low)

        encode(2 + q, low, o)
        return carry

    lax.fori_loop(0, 4, near_half, 0)
    swapped(chip).wait_recv()
    for cols in tiles:
        add_days(chip, whole, cols, transform(chip, whole, cols))

    def arrive(piece, carry):
        turn = piece + jnp.where(piece // 2 == 2, 1, 0)
        shipped(piece, 1).wait_recv()
        decode(piece, pl.ds(pl.multiple_of((turn % 2) * part, part), part))
        return carry

    lax.fori_loop(2, pieces, arrive, 0)
    real, imag = sums[1, :, :lag_count], sums[2, :, :lag_count]
    linear_ref[...] = sums[0, :, :lag_count]
    power_ref[...] = real * real + imag * imag

    mask_copy.wait_send()
    for g in range(chips):
        swapped(g).wait_send()
    for o in range(1, peers + 1):
        told(o).wait_send()
    for piece in range(pieces):
        shipped(piece, 1).wait_send()


def shards(correlations, mask, counts):
    days, pairs, lag_count = correlations.shape
    groups = lax.axis_size("day")
    chips = groups // 2
    owned = pairs // groups
    width = padded(lag_count)
    peers = 2 * lax.axis_size("pair") - 1

    strip = jnp.asarray(kernel_strip(lag_count))
    size = width + width // 2 + 128
    pieces = 2 * chips - 2
    out = jax.ShapeDtypeStruct((owned, lag_count), jnp.float32)
    vmem = pl.BlockSpec(memory_space=pltpu.VMEM)
    hbm = pl.BlockSpec(memory_space=pl.ANY)
    dma = pltpu.SemaphoreType.DMA
    linear_sum, power = pl.pallas_call(
        functools.partial(stack_kernel, lag_count),
        in_specs=[hbm, vmem, hbm],
        out_specs=(vmem, vmem),
        out_shape=(out, out),
        scratch_shapes=[
            pltpu.VMEM((chips, 2 * days, owned, lag_count), jnp.bfloat16),
            pltpu.VMEM((chips, days, owned, lag_count), jnp.bfloat16),
            pltpu.VMEM(strip.shape, jnp.bfloat16),
            pltpu.VMEM((width, width), jnp.bfloat16),
            pltpu.VMEM((3, owned, width), jnp.float32),
            pltpu.VMEM((2 * days * owned, width), jnp.float32),
            pltpu.VMEM((days, pairs), jnp.int32),
            pltpu.VMEM((pairs, 2 * days), jnp.float32),
            pltpu.VMEM((chips, 2 * days, owned, 1), jnp.float32),
            pltpu.VMEM((2 * days, owned, 1), jnp.float32),
            pltpu.VMEM((2 * days, 256), jnp.float32),
            pltpu.VMEM((peers, 2 * days, 256), jnp.float32),
            pltpu.VMEM((pieces, owned // 2, size), jnp.int32),
            pltpu.VMEM((pieces, owned // 2, size), jnp.int32),
            dma((chips,)), dma((chips,)), dma, dma((chips,)), dma((chips,)), dma, dma,
            dma((peers,)), dma((peers,)), dma((pieces,)), dma((pieces,)),
        ],
        compiler_params=pltpu.CompilerParams(
            vmem_limit_bytes=46 * 2**20, collective_id=0, has_side_effects=True
        ),
        name="stack",
    )(correlations.reshape(days, groups, owned, lag_count), mask, strip)
    inverse = (1.0 / jnp.maximum(counts.astype(jnp.float32), 1.0))[:, None]
    linear = linear_sum * inverse
    return (linear * (power * (inverse * inverse)), linear)


def solution(mesh):
    placed = (P("day", "pair", None), P("day", "pair"), P(("pair", "day")))
    return jax.shard_map(
        shards,
        mesh=mesh,
        in_specs=placed,
        out_specs=(P(("pair", "day"), None), P(("pair", "day"), None)),
        check_vma=False,
    )
```
